32 devices in a mesh: pw: 8 (over z, core), band: 4 (over y, x).
Axes of the slice: x: 2, y: 2, z: 4, core: 2. Of those that a mesh axis runs over, the one named last changes fastest.
Arguments:
- wavefunctions: bfloat16 [2, 4096, 512], P(None, 'pw', 'band'), may hold values from -0.09375 to 0.09375
- miller: int32 [3, 4096], P(None, 'pw'), may hold values from -16 to 16
- reciprocal: float32 [3, 3], replicated, may hold values from -0.15 to 1.15, as said below
- fractional: float32 [3, 32], replicated, may hold values from 0 to 1
- species: int32 [32], replicated, may hold values from 0 to 3
- atom_order: int32 [32], replicated, may hold values from 0 to 31, each once
- radial_widths: float32 [4, 4], replicated, may hold values from 0.003 to 0.02
- onsite_base: float32 [4, 8, 8], replicated, may hold values from -2 to 2
- coupling: float32 [4, 64, 64], replicated, may hold values from -0.75 to 0.75
- occupations: float32 [512], P('band'), may hold values from 0 to 3, as said below
Outputs:
- applied: bfloat16 [2, 4096, 512], P(None, 'pw', 'band')
- onsite_d: float32 [32, 8, 8], P('pw')
The draws below stay inside these ranges and needn't reach their ends.
Inputs may be any that keep to these rules, and one draw needn't show every extreme that they name: `atom_order`: a permutation of the atoms. `reciprocal`: each diagonal entry is 0.85 or more and each other entry 0.15 or less in magnitude. `occupations`: positive.
All inputs are finite; a program needn't handle non-finite values.
Results may differ from the reference program's by a relative error of at most 0.008.
Values may be sent and summed in bfloat16 or wider, within the bound.
A program may use at most 64 MiB of HBM per device.

```python
import math
import jax
import jax.numpy as jnp
from jax import lax

PROJ = 8
SPECIES = 4
NPW = 4096
NBANDS = 512
ATOMS = 32


def draw_occupations(key, part):
    position = jnp.arange(NBANDS, dtype=jnp.float32) / NBANDS
    fermi = 2.0 / (1.0 + jnp.exp((position - 0.8) * 6.0))
    noise = jax.random.uniform(key, (NBANDS,), jnp.float32, 0.8, 1.2)
    return fermi * noise


def draw_reciprocal(key, part):
    offsets = 0.05 * jax.random.truncated_normal(key, -3.0, 3.0, (3, 3), jnp.float32)
    return jnp.eye(3, dtype=jnp.float32) + offsets


def set_ends(drawn, key, least, largest):
    shape = drawn.shape
    index_at = [jax.random.randint(jax.random.fold_in(key, axis), (), 0, shape[axis]) for axis in range(len(shape))]
    drawn = drawn.at[tuple(index_at)].set(least)
    longest = shape.index(max(shape))
    index_at[longest] = (index_at[longest] + 1) % shape[longest]
    return drawn.at[tuple(index_at)].set(largest)


def levels(stream_key, extent, split, low, high):
    loudness, own = 1.0, jax.random.fold_in(stream_key, 6)
    for dim, parts in split:
        steps = jnp.exp(jax.random.uniform(jax.random.fold_in(own, dim), (parts,), jnp.float32, low / len(split), high / len(split)))
        loudness = loudness * jnp.repeat(steps, extent[dim] // parts).reshape([-1 if axis == dim else 1 for axis in range(len(extent))])
    return loudness


def scatter_about(own_key, shape, deviation, bound, pieces=(), kind=jnp.bfloat16):
    factor_of = levels(own_key, shape, pieces, -0.22, 0.18) if pieces else 1.0
    values = jax.random.normal(own_key, shape, jnp.float32) * deviation * factor_of
    return jnp.minimum(jnp.maximum(values, -bound), bound).astype(kind)


def setup_inputs(seed: int = 0) -> dict:
    arg_keys = jax.random.split(jax.random.key(seed), 11)
    wavefunctions = scatter_about(arg_keys[0], (2, NPW, NBANDS), NPW ** -0.5, 0.09375, ((1, 8), (2, 4)))
    miller = set_ends(jax.random.randint(arg_keys[1], (3, NPW), -16, 17), jax.random.fold_in(arg_keys[1], 1), -16, 16).astype(jnp.int32)
    reciprocal = draw_reciprocal(jax.random.fold_in(arg_keys[10], 71), 0)
    fractional = jnp.clip(jax.random.uniform(arg_keys[3], (3, ATOMS), jnp.float32, 0.0, 1.0), 0.0, 1.0)
    species = set_ends(jax.random.randint(arg_keys[4], (ATOMS,), 0, SPECIES), jax.random.fold_in(arg_keys[4], 1), 0, SPECIES - 1).astype(jnp.int32)
    atom_order = jax.random.permutation(arg_keys[5], ATOMS).astype(jnp.int32)
    radial_widths = jnp.clip(jnp.exp(jax.random.uniform(arg_keys[6], (SPECIES, 4), jnp.float32, math.log(0.003), math.log(0.02))), 0.003, 0.02)
    onsite_base = scatter_about(arg_keys[7], (SPECIES, PROJ, PROJ), PROJ ** -0.5, 2.0, (), jnp.float32)
    coupling = scatter_about(arg_keys[8], (SPECIES, PROJ * PROJ, PROJ * PROJ), (PROJ * PROJ) ** -0.5, 0.75, (), jnp.float32)
    occupations = draw_occupations(jax.random.fold_in(arg_keys[10], 71), 0)
    return {"wavefunctions": wavefunctions, "miller": miller, "reciprocal": reciprocal, "fractional": fractional, "species": species, "atom_order": atom_order, "radial_widths": radial_widths, "onsite_base": onsite_base, "coupling": coupling, "occupations": occupations}


HIGH = lax.Precision.HIGHEST


def projector_tile(miller_cols, reciprocal, positions, atom_species, radial_widths):
    two_pi = 2.0 * math.pi
    miller_real = miller_cols.astype(jnp.float32)
    g_vectors = two_pi * jnp.dot(reciprocal, miller_real, precision=HIGH)
    g_square = jnp.sum(g_vectors * g_vectors, axis=0)
    phases = two_pi * jnp.dot(positions.T, miller_real, precision=HIGH)
    onehot = (atom_species[:, None] == jnp.arange(radial_widths.shape[0], dtype=jnp.int32)[None, :]).astype(jnp.float32)
    widths = jnp.dot(onehot, radial_widths, precision=HIGH)
    radial = jnp.exp(-0.5 * g_square[None, None, :] * (widths * widths)[:, :, None])
    s_part = radial[:, 0:2, :]
    p_first = g_vectors[None, :, :] * (widths[:, 2, None, None] * radial[:, 2:3, :])
    p_second = g_vectors[None, :, :] * (widths[:, 3, None, None] * radial[:, 3:4, :])
    p_part = jnp.concatenate([p_first, p_second], axis=1)
    cosine = jnp.cos(phases)[:, None, :]
    sine = jnp.sin(phases)[:, None, :]
    beta_real = jnp.concatenate([s_part * cosine, -p_part * sine], axis=1)
    beta_imag = jnp.concatenate([-s_part * sine, -p_part * cosine], axis=1)
    rows = positions.shape[1] * 8
    return (beta_real.reshape(rows, -1).astype(jnp.bfloat16), beta_imag.reshape(rows, -1).astype(jnp.bfloat16))


def project(beta_real, beta_imag, wave_real, wave_imag):
    proj_real = jnp.dot(beta_real, wave_real, preferred_element_type=jnp.float32) + jnp.dot(beta_imag, wave_imag, preferred_element_type=jnp.float32)
    proj_imag = jnp.dot(beta_real, wave_imag, preferred_element_type=jnp.float32) - jnp.dot(beta_imag, wave_real, preferred_element_type=jnp.float32)
    return jnp.stack([proj_real, proj_imag], axis=1)


def occupancy_terms(projections, weights):
    grouped = projections.reshape(projections.shape[0] // 8, 8, 2, projections.shape[2])
    return jnp.einsum("aicn,ajcn,n->aij", grouped, grouped, weights, precision=HIGH)


def onsite_matrix(occupancy, atom_species, onsite_base, coupling):
    count = occupancy.shape[0]
    kinds = onsite_base.shape[0]
    onehot = (atom_species[:, None] == jnp.arange(kinds, dtype=jnp.int32)[None, :]).astype(jnp.float32)
    response = jnp.einsum("skl,al->ask", coupling, occupancy.reshape(count, 64), precision=HIGH)
    base = jnp.einsum("as,sk->ak", onehot, onsite_base.reshape(kinds, 64), precision=HIGH)
    total = base + jnp.einsum("as,ask->ak", onehot, response, precision=HIGH)
    return total.reshape(count, 8, 8)


def weigh(onsite, projections):
    grouped = projections.reshape(projections.shape[0] // 8, 8, 2, projections.shape[2])
    weighted = jnp.einsum("aij,ajcn->aicn", onsite, grouped, precision=HIGH)
    return weighted.reshape(projections.shape).astype(jnp.bfloat16)


def back_project(beta_real, beta_imag, weighted):
    dims = (((0,), (0,)), ((), ()))
    q_real = weighted[:, 0, :]
    q_imag = weighted[:, 1, :]
    out_real = lax.dot_general(beta_real, q_real, dims, preferred_element_type=jnp.float32) - lax.dot_general(beta_imag, q_imag, dims, preferred_element_type=jnp.float32)
    out_imag = lax.dot_general(beta_real, q_imag, dims, preferred_element_type=jnp.float32) + lax.dot_general(beta_imag, q_real, dims, preferred_element_type=jnp.float32)
    return jnp.stack([out_real, out_imag], axis=0)


def reference(wavefunctions, miller, reciprocal, fractional, species, atom_order, radial_widths, onsite_base, coupling, occupations):
    sorted_species = species[atom_order]
    sorted_positions = fractional[:, atom_order]
    beta_real, beta_imag = projector_tile(miller, reciprocal, sorted_positions, sorted_species, radial_widths)
    projections = project(beta_real, beta_imag, wavefunctions[0], wavefunctions[1])
    weights = occupations / NBANDS
    occupancy = occupancy_terms(projections, weights)
    onsite = onsite_matrix(occupancy, sorted_species, onsite_base, coupling)
    weighted = weigh(onsite, projections)
    applied = back_project(beta_real, beta_imag, weighted).astype(jnp.bfloat16)
    return applied, onsite
```

```python
import functools
import math

import jax
import jax.numpy as jnp
import numpy as np
from jax import lax
from jax.experimental import pallas as pl
from jax.experimental.pallas import tpu as pltpu
from jax.sharding import PartitionSpec as P

MESH = pl.DeviceIdType.MESH
HIGH = lax.Precision.HIGHEST
BF = jnp.bfloat16
F32 = jnp.float32


def even_fit(function, degree):
    nodes = 0.125 + 0.125 * np.cos(np.pi * (np.arange(64) + 0.5) / 64)
    fit = np.polynomial.Chebyshev.fit(nodes, function(np.sqrt(nodes)), degree, domain=[0.0, 0.25])
    return [float(c) for c in fit.convert(kind=np.polynomial.Polynomial, domain=[-1, 1]).coef]


COS = even_fit(lambda t: np.cos(2 * np.pi * t), 7)
SIN = even_fit(lambda t: np.sin(2 * np.pi * t) / t, 7)


def series(coefs, u):
    value = jnp.full_like(u, coefs[-1])
    for c in coefs[-2::-1]:
        value = value * u + c
    return value


def iota(shape, dim):
    return lax.broadcasted_iota(jnp.int32, shape, dim)


def kernel(
    n,
    nb,
    wave,
    miller_h,
    reciprocal_h,
    fractional_h,
    species_h,
    order_h,
    widths_h,
    base_h,
    coupling_h,
    occ_h,
    applied,
    onsite,
    miller,
    reciprocal,
    fractional,
    species,
    order,
    widths,
    base,
    coupling,
    occ,
    wv,
    xs,
    cs,
    sn,
    amp,
    beta,
    beta_t,
    part,
    rs_in,
    p_all,
    o_in,
    o_sum,
    spread,
    turned,
    respond_t,
    respond,
    bare,
    folded,
    ww,
    load_sem,
    rs_s,
    rs_r,
    ag_s,
    ag_r,
    oc_s,
    oc_r,
    ready,
):
    me = lax.axis_index("pw")
    mb = lax.axis_index("band")
    npw = wave.shape[1]
    bands = wave.shape[2]
    atoms = order.shape[0]
    kinds = widths.shape[0]
    own = atoms // n
    rows = own * 8
    every = atoms * 8
    peers = n * nb

    small = [
        (miller_h, miller),
        (reciprocal_h, reciprocal),
        (fractional_h, fractional),
        (species_h, species),
        (order_h, order),
        (widths_h, widths),
        (base_h, base),
        (coupling_h, coupling),
        (occ_h, occ),
        (wave.at[0], wv.at[pl.ds(0, npw), pl.ds(0, bands)]),
        (wave.at[1], wv.at[pl.ds(0, npw), pl.ds(bands, bands)]),
        (wave.at[1], wv.at[pl.ds(npw, npw), pl.ds(0, bands)]),
    ]
    loads = [
        pltpu.make_async_copy(source, to, load_sem.at[i]) for i, (source, to) in enumerate(small)
    ]
    for copy in loads:
        copy.start()
    barrier = pltpu.get_barrier_semaphore()

    for d in range(1, n):
        pl.semaphore_signal(
            barrier, inc=1, device_id={"pw": lax.rem(me + d, n)}, device_id_type=MESH
        )
    for b in range(1, nb):
        pl.semaphore_signal(
            barrier, inc=1, device_id={"band": lax.rem(mb + b, nb)}, device_id_type=MESH
        )
    for copy in loads[0:6]:
        copy.wait()

    m = [miller[c : c + 1, :].astype(F32) for c in range(3)]
    g = [
        (2.0 * math.pi)
        * (reciprocal[c, 0] * m[0] + reciprocal[c, 1] * m[1] + reciprocal[c, 2] * m[2])
        for c in range(3)
    ]
    g2 = g[0] * g[0] + g[1] * g[1] + g[2] * g[2]
    j = iota((8, npw), 0)
    is_s = j < 2
    wide = [jnp.broadcast_to(v, (8, npw)) for v in g]
    factor = jnp.where(
        (j == 2) | (j == 5), wide[0], jnp.where((j == 3) | (j == 6), wide[1], wide[2])
    )
    half = jnp.broadcast_to(-0.5 * g2, (8, npw))
    for s in range(widths.shape[0]):
        w = jnp.where(
            j == 0,
            widths[s, 0],
            jnp.where(j == 1, widths[s, 1], jnp.where(j < 5, widths[s, 2], widths[s, 3])),
        )
        amp[s] = jnp.where(is_s, 1.0, factor * w) * jnp.exp(half * (w * w))

    def position(k, carry):
        a = order[k]
        xs[pl.ds(k, 1), :] = (
            fractional[0, a] * m[0] + fractional[1, a] * m[1] + fractional[2, a] * m[2]
        )
        return carry

    lax.fori_loop(0, atoms, position, 0, unroll=8)
    x = xs[...]
    t = x - jnp.round(x)
    u = t * t
    cs[...] = series(COS, u)
    sn[...] = t * series(SIN, u)

    def projector(pair, carry):
        real, imag = [], []
        for e in range(2):
            k = pair * 2 + e
            c = jnp.broadcast_to(cs[pl.ds(k, 1), :], (8, npw))
            s = jnp.broadcast_to(sn[pl.ds(k, 1), :], (8, npw))
            a = amp[species[order[k]]]
            real.append(a * jnp.where(is_s, c, -s))
            imag.append(-a * jnp.where(is_s, s, c))
        at = pl.ds(pl.multiple_of(pair * 16, 16), 16)
        beta[at, 0:npw] = jnp.concatenate(real, axis=0).astype(BF)
        beta[at, npw : 2 * npw] = jnp.concatenate(imag, axis=0).astype(BF)
        return carry

    lax.fori_loop(0, atoms // 2, projector, 0, unroll=4)

    for copy in loads[6:]:
        copy.wait()
    wv[npw : 2 * npw, bands : 2 * bands] = -wv[0:npw, 0:bands]
    part[...] = jnp.dot(beta[...], wv[...], preferred_element_type=F32).astype(BF)
    pl.semaphore_wait(barrier, n - 1 + nb - 1)

    def block(index):
        return pl.ds(pl.multiple_of(index * rows, rows), rows)

    def scatter(s):
        to = lax.rem(me + s, n)
        return pltpu.make_async_remote_copy(
            src_ref=part.at[block(to)],
            dst_ref=rs_in.at[s],
            send_sem=rs_s.at[s],
            recv_sem=rs_r.at[s],
            device_id={"pw": to},
            device_id_type=MESH,
        )

    upper_half = me // (n // 2)
    far_first = [
        lax.rem(n - 2 - me + upper_half + (2 * upper_half - 1) * i + 2 * (n - 1), n - 1) + 1
        for i in range(n - 1)
    ]
    sends = [scatter(s) for s in range(1, n)]
    for s in far_first:
        scatter(s).start()
    for b in range(1, nb):
        pl.semaphore_signal(
            ready, inc=1, device_id={"band": lax.rem(mb + b, nb)}, device_id_type=MESH
        )

    beta_t[:, 0:every] = beta[:, 0:npw].T
    beta_t[:, every : 2 * every] = beta[:, npw : 2 * npw].T
    weights = occ[...] * (1.0 / (bands * nb))
    weights = jnp.concatenate([weights, weights], axis=1)
    group = min(atoms, 32)
    span = group * 8
    fan = (iota((8, span), 1) % 8 == iota((8, span), 0)).astype(F32)
    diagonal = iota((span, span), 0) // 8 == iota((span, span), 1) // 8
    fold = (iota((span, 8), 0) % 8 == iota((span, 8), 1)).astype(F32)
    slot = [iota((8, 128), 0) == 2 * t + iota((8, 128), 1) // 64 for t in range(4)]
    for kind in range(kinds):
        spread[kind] = jnp.dot(base[kind], fan, precision=HIGH, preferred_element_type=F32)
        for t in range(4):
            turned[kind, :, t * 128 : t * 128 + 128] = jnp.concatenate(
                [coupling[kind, i * 8 : i * 8 + 8, :] for i in (2 * t, 2 * t + 1)], axis=1
            )

    def expand(pair, carry):
        kind = [species[order[pair * 2 + e]] for e in range(2)]
        at = pl.ds(pl.multiple_of(pair * 16, 16), 16)
        respond_t[at, :] = jnp.concatenate([turned[s] for s in kind], axis=0).astype(BF)
        bare[at, :] = jnp.concatenate([spread[s] for s in kind], axis=0)
        return carry

    lax.fori_loop(0, atoms // 2, expand, 0, unroll=4)
    for q in range(0, every, span):
        respond[:, q : q + span] = respond_t[q : q + span, :].T

    pl.semaphore_wait(ready, nb - 1)
    total = part[block(me), :].astype(F32)
    for s in range(1, n):
        sends[s - 1].wait_recv()
        total = total + rs_in[s].astype(F32)
    p_all[block(me), :] = total.astype(BF)
    pairs = []
    for k in range(own):
        left = total[k * 8 : k * 8 + 8, :] * weights
        pair = jnp.concatenate(
            [jnp.broadcast_to(total[k * 8 + i : k * 8 + i + 1, :], (8, 2 * bands)) * left for i in range(8)], axis=0
        ).astype(BF)
        pairs += [pair, pair]
    flat = lax.dot_general(
        jnp.ones((16, 2 * bands), BF),
        jnp.concatenate(pairs, axis=0),
        (((1,), (1,)), ((), ())),
        preferred_element_type=F32,
    )
    for k in range(own):
        o_in[mb, me, k : k + 1, :] = flat[0:1, k * 128 : k * 128 + 128]

    def skip(i, at, size):
        return i + (i + size - at) // size

    def occupancy_copy(to, band, by_owner, by_band, at):
        return pltpu.make_async_remote_copy(
            src_ref=o_in.at[mb, me],
            dst_ref=o_in.at[mb, me],
            send_sem=oc_s.at[at],
            recv_sem=oc_r.at[by_owner * nb + by_band],
            device_id={"pw": to, "band": band},
            device_id_type=MESH,
        )

    def away(i, j):
        return skip(i, me, n), j

    def near(j):
        return me, skip(j, mb, nb)

    def each_peer(step):
        if peers <= 64:
            for i in range(n - 1):
                for j in range(nb):
                    step(*away(i, j), i * nb + j)
        else:
            lax.fori_loop(
                0, (n - 1) * nb, lambda q, c: (step(*away(q // nb, lax.rem(q, nb)), q), c)[1], 0
            )
        for j in range(nb - 1):
            step(*near(j), (n - 1) * nb + j)

    each_peer(lambda to, band, at: occupancy_copy(to, band, me, mb, at).start())
    p_sends = []
    for i in range(n - 1):
        to = skip(i, me, n)
        copy = pltpu.make_async_remote_copy(
            src_ref=p_all.at[block(me)],
            dst_ref=p_all.at[block(me)],
            send_sem=ag_s.at[i],
            recv_sem=ag_r.at[me],
            device_id={"pw": to},
            device_id_type=MESH,
        )
        copy.start()
        p_sends.append(copy)

    each_peer(lambda to, band, at: occupancy_copy(to, band, to, band, at).wait_recv())
    for d in range(n):
        summed = o_in[0, d]
        for b in range(1, nb):
            summed = summed + o_in[b, d]
        o_sum[d * own : d * own + own, :] = summed
    matrix = []
    for q in range(0, atoms, group):
        lines = []
        for k in range(q, q + group):
            line = jnp.broadcast_to(o_sum[k : k + 1, :], (8, 128))
            lines.append(
                jnp.concatenate([jnp.where(slot[t], line, 0.0) for t in range(4)], axis=1)
            )
        lines = jnp.concatenate(lines, axis=0).astype(BF)
        answer = jnp.dot(
            lines, respond[:, q * 8 : q * 8 + span], preferred_element_type=F32
        )
        answer = jnp.where(diagonal, answer + bare[q * 8 : q * 8 + span, :], 0.0)
        folded[q * 8 : q * 8 + span, :] = answer
        matrix.append(answer.astype(BF))
    for s in range(1, n):
        owner = lax.rem(me + s, n)
        pltpu.make_async_remote_copy(
            src_ref=p_all.at[block(owner)],
            dst_ref=p_all.at[block(owner)],
            send_sem=ag_s.at[0],
            recv_sem=ag_r.at[owner],
            device_id={"pw": owner},
            device_id_type=MESH,
        ).wait_recv()
    for q in range(0, every, span):
        w = jnp.dot(matrix[q // span], p_all[q : q + span, :], preferred_element_type=F32)
        w = w.astype(BF)
        ww[q : q + span, :] = w
        ww[every + q : every + q + span, 0:bands] = -w[:, bands : 2 * bands]
        ww[every + q : every + q + span, bands : 2 * bands] = w[:, 0:bands]
    result = jnp.dot(beta_t[...], ww[...], preferred_element_type=F32).astype(BF)
    applied[0] = result[:, 0:bands]
    applied[1] = result[:, bands : 2 * bands]
    mine = jnp.dot(folded[block(me), :], fold, precision=HIGH, preferred_element_type=F32)
    for k in range(own):
        onsite[k] = mine[k * 8 : k * 8 + 8, :]
    for copy in sends + p_sends:
        copy.wait_send()
    each_peer(lambda to, band, at: occupancy_copy(to, band, me, mb, at).wait_send())


def finish(applied_in, onsite_in, applied, onsite, sem):
    copies = [
        pltpu.make_async_copy(applied_in, applied, sem.at[0]),
        pltpu.make_async_copy(onsite_in, onsite, sem.at[1]),
    ]
    for copy in copies:
        copy.start()
    for copy in copies:
        copy.wait()


def solution(mesh):
    n, nb = mesh.shape["pw"], mesh.shape["band"]

    def local(wave, miller, reciprocal, fractional, species, order, widths, base, coupling, occ):
        _, npw, bands = wave.shape
        atoms = order.shape[0]
        own = atoms // n
        rows, every = own * 8, atoms * 8
        span = min(atoms, 32) * 8
        kinds = widths.shape[0]
        vmem = pl.BlockSpec(memory_space=pltpu.VMEM)
        hbm = pl.BlockSpec(memory_space=pltpu.HBM)
        dma = pltpu.SemaphoreType.DMA
        results = (
            jax.ShapeDtypeStruct(wave.shape, BF),
            jax.ShapeDtypeStruct((own, 8, 8), F32),
        )
        first = pl.pallas_call(
            functools.partial(kernel, n, nb),
            out_shape=results,
            in_specs=[hbm] * 10,
            out_specs=(vmem, vmem),
            scratch_shapes=[
                pltpu.VMEM(miller.shape, jnp.int32),
                pltpu.SMEM(reciprocal.shape, F32),
                pltpu.SMEM(fractional.shape, F32),
                pltpu.SMEM(species.shape, jnp.int32),
                pltpu.SMEM(order.shape, jnp.int32),
                pltpu.SMEM(widths.shape, F32),
                pltpu.VMEM(base.shape, F32),
                pltpu.VMEM(coupling.shape, F32),
                pltpu.VMEM((1, bands), F32),
                pltpu.VMEM((2 * npw, 2 * bands), BF),
                pltpu.VMEM((atoms, npw), F32),
                pltpu.VMEM((atoms, npw), F32),
                pltpu.VMEM((atoms, npw), F32),
                pltpu.VMEM((kinds, 8, npw), F32),
                pltpu.VMEM((every, 2 * npw), BF),
                pltpu.VMEM((npw, 2 * every), BF),
                pltpu.VMEM((every, 2 * bands), BF),
                pltpu.VMEM((n, rows, 2 * bands), BF),
                pltpu.VMEM((every, 2 * bands), BF),
                pltpu.VMEM((nb, n, own, 128), F32),
                pltpu.VMEM((atoms, 128), F32),
                pltpu.VMEM((kinds, 8, span), F32),
                pltpu.VMEM((kinds, 8, 512), F32),
                pltpu.VMEM((every, 512), BF),
                pltpu.VMEM((512, every), BF),
                pltpu.VMEM((every, span), F32),
                pltpu.VMEM((every, span), F32),
                pltpu.VMEM((2 * every, 2 * bands), BF),
                dma((12,)),
                dma((n,)),
                dma((n,)),
                dma((n,)),
                dma((n,)),
                dma((n * nb,)),
                dma((n * nb,)),
                pltpu.SemaphoreType.REGULAR,
            ],
            compiler_params=pltpu.CompilerParams(
                collective_id=0, has_side_effects=True, vmem_limit_bytes=40 * 2**20
            ),
        )(
            *[
                pltpu.with_memory_space_constraint(value, pltpu.HBM)
                for value in (
                    wave,
                    miller,
                    reciprocal,
                    fractional,
                    species,
                    order,
                    widths,
                    base,
                    coupling,
                    occ.reshape(1, bands),
                )
            ]
        )
        anywhere = pl.BlockSpec(memory_space=pl.ANY)
        return pl.pallas_call(
            finish,
            out_shape=results,
            in_specs=[anywhere] * 2,
            out_specs=(hbm, hbm),
            scratch_shapes=[dma((2,))],
            compiler_params=pltpu.CompilerParams(vmem_limit_bytes=2**20),
        )(*first)

    placed = (P(None, "pw", "band"), P(None, "pw"), P(), P(), P(), P(), P(), P(), P(), P("band"))
    return jax.shard_map(
        local,
        mesh=mesh,
        in_specs=placed,
        out_specs=(P(None, "pw", "band"), P("pw", None, None)),
        check_vma=False,
    )
```

```python
import functools
import math

import jax
import jax.numpy as jnp
import numpy as np
from jax import lax
from jax.experimental import pallas as pl
from jax.experimental.pallas import tpu as pltpu
from jax.sharding import PartitionSpec as P

MESH = pl.DeviceIdType.MESH
HIGH = lax.Precision.HIGHEST
BF = jnp.bfloat16
F32 = jnp.float32


def even_fit(function, degree):
    nodes = 0.125 + 0.125 * np.cos(np.pi * (np.arange(64) + 0.5) / 64)
    fit = np.polynomial.Chebyshev.fit(nodes, function(np.sqrt(nodes)), degree, domain=[0.0, 0.25])
    return [float(c) for c in fit.convert(kind=np.polynomial.Polynomial, domain=[-1, 1]).coef]


COS = even_fit(lambda t: np.cos(2 * np.pi * t), 7)
SIN = even_fit(lambda t: np.sin(2 * np.pi * t) / t, 7)


def series(coefs, u):
    value = jnp.full_like(u, coefs[-1])
    for c in coefs[-2::-1]:
        value = value * u + c
    return value


def iota(shape, dim):
    return lax.broadcasted_iota(jnp.int32, shape, dim)


def kernel(
    n,
    nb,
    wave,
    miller_h,
    reciprocal_h,
    fractional_h,
    species_h,
    order_h,
    widths_h,
    base_h,
    coupling_h,
    occ_h,
    applied,
    onsite,
    miller,
    reciprocal,
    fractional,
    species,
    order,
    widths,
    base,
    coupling,
    occ,
    wv,
    xs,
    cs,
    sn,
    amp,
    beta,
    beta_t,
    part,
    kept,
    pair_in,
    pair_sum,
    rs_in,
    p_all,
    o_in,
    o_sum,
    spread,
    turned,
    respond_t,
    respond,
    bare,
    folded,
    ww,
    load_sem,
    sw_s,
    sw_r,
    rs_s,
    rs_r,
    ag_s,
    ag_r,
    oc_s,
    oc_r,
    ready,
    here,
    here_b,
    go,
):
    me = lax.axis_index("pw")
    mb = lax.axis_index("band")
    npw = wave.shape[1]
    bands = wave.shape[2]
    atoms = order.shape[0]
    kinds = widths.shape[0]
    own = atoms // n
    rows = own * 8
    every = atoms * 8
    peers = n * nb
    chips = n // 2
    half = chips * rows
    chip, side = me // 2, lax.rem(me, 2)
    mate = me + 1 - 2 * side
    single, double = chips // 2, chips // 4
    chunk = 2 * rows

    def handled(z):
        return 1 if z < single else 2 if z < single + double else 0

    def first_slot(z):
        return z if z < single else 2 * z - single

    def atom_at(k):
        return order[(2 * (k // own % chips) + k // own // chips) * own + k % own]

    small = [
        (miller_h, miller),
        (reciprocal_h, reciprocal),
        (fractional_h, fractional),
        (species_h, species),
        (order_h, order),
        (widths_h, widths),
        (base_h, base),
        (coupling_h, coupling),
        (occ_h, occ),
        (wave.at[0], wv.at[pl.ds(0, npw), pl.ds(0, bands)]),
        (wave.at[1], wv.at[pl.ds(0, npw), pl.ds(bands, bands)]),
        (wave.at[1], wv.at[pl.ds(npw, npw), pl.ds(0, bands)]),
    ]
    loads = [
        pltpu.make_async_copy(source, to, load_sem.at[i]) for i, (source, to) in enumerate(small)
    ]
    for copy in loads:
        copy.start()
    barrier = pltpu.get_barrier_semaphore()
    others = [lax.rem(me + d, n) for d in range(1, n)]
    group_bands = [lax.rem(mb + d, nb) for d in range(1, nb)]

    hub = n // 2 - 1

    def greet(sem, later):
        for to in others:
            @pl.when(to > me if later else to < me)
            def _():
                pl.semaphore_signal(
                    sem(0), inc=1, device_id={"pw": to}, device_id_type=MESH
                )

        @pl.when(me == hub)
        def _():
            for to in group_bands:
                @pl.when(to > mb if later else to < mb)
                def _():
                    pl.semaphore_signal(
                        sem(1), inc=1, device_id={"band": to}, device_id_type=MESH
                    )

    greet(lambda axis: barrier, True)
    @pl.when(jnp.logical_and(me > 0, me != hub))
    def _():
        pl.semaphore_wait(barrier, me)

    @pl.when(me == hub)
    def _():
        pl.semaphore_wait(barrier, hub + mb)

    greet(lambda axis: here_b if axis else here.at[me], False)
    for copy in loads[0:6]:
        copy.wait()

    m = [miller[c : c + 1, :].astype(F32) for c in range(3)]
    g = [
        (2.0 * math.pi)
        * (reciprocal[c, 0] * m[0] + reciprocal[c, 1] * m[1] + reciprocal[c, 2] * m[2])
        for c in range(3)
    ]
    g2 = g[0] * g[0] + g[1] * g[1] + g[2] * g[2]
    j = iota((8, npw), 0)
    is_s = j < 2
    wide = [jnp.broadcast_to(v, (8, npw)) for v in g]
    factor = jnp.where(
        (j == 2) | (j == 5), wide[0], jnp.where((j == 3) | (j == 6), wide[1], wide[2])
    )
    decay = jnp.broadcast_to(-0.5 * g2, (8, npw))
    for s in range(widths.shape[0]):
        w = jnp.where(
            j == 0,
            widths[s, 0],
            jnp.where(j == 1, widths[s, 1], jnp.where(j < 5, widths[s, 2], widths[s, 3])),
        )
        amp[s] = jnp.where(is_s, 1.0, factor * w) * jnp.exp(decay * (w * w))

    def at_row(start, size):
        return pl.ds(pl.multiple_of(start, rows), size)

    def scatter(z):
        size = handled(z) * rows
        return pltpu.make_async_remote_copy(
            src_ref=pair_sum.at[pl.ds(first_slot(z) * rows, size)],
            dst_ref=rs_in.at[chip, pl.ds(0, size)],
            send_sem=rs_s.at[z],
            recv_sem=rs_r.at[chip],
            device_id={"pw": 2 * z + side},
            device_id_type=MESH,
        )

    def swap(c):
        return pltpu.make_async_remote_copy(
            src_ref=part.at[pl.ds(c, chunk)],
            dst_ref=pair_in.at[pl.ds(c, chunk)],
            send_sem=sw_s.at[c // chunk],
            recv_sem=sw_r.at[c // chunk],
            device_id={"pw": mate},
            device_id_type=MESH,
        )

    def projectors(which, c):
        first = (c // rows) * 2 * own + which * own
        at = c // 8
        atom = [
            order[first + (k // own) * 2 * own + k % own] for k in range(chunk // 8)
        ]
        for k, a in enumerate(atom):
            xs[at + k : at + k + 1, :] = (
                fractional[0, a] * m[0] + fractional[1, a] * m[1] + fractional[2, a] * m[2]
            )
        x = xs[at : at + chunk // 8, :]
        t = x - jnp.round(x)
        u = t * t
        cs[at : at + chunk // 8, :] = series(COS, u)
        sn[at : at + chunk // 8, :] = t * series(SIN, u)
        for pair in range(chunk // 16):
            real, imag = [], []
            for k in (2 * pair, 2 * pair + 1):
                c_k = jnp.broadcast_to(cs[at + k : at + k + 1, :], (8, npw))
                s_k = jnp.broadcast_to(sn[at + k : at + k + 1, :], (8, npw))
                a_k = amp[species[atom[k]]]
                real.append(a_k * jnp.where(is_s, c_k, -s_k))
                imag.append(-a_k * jnp.where(is_s, s_k, c_k))
            to = pl.ds(pl.multiple_of(which * half + c + pair * 16, 16), 16)
            beta[to, 0:npw] = jnp.concatenate(real, axis=0).astype(BF)
            beta[to, npw : 2 * npw] = jnp.concatenate(imag, axis=0).astype(BF)

    steps = [(1 - side, c, True) for c in range(0, half, chunk)]
    steps += [(side, c, False) for c in range(0, half, chunk)]
    projectors(*steps[0][:2])
    for copy in loads[6:]:
        copy.wait()
    wv[npw : 2 * npw, bands : 2 * bands] = -wv[0:npw, 0:bands]
    for index, (which, c, away) in enumerate(steps):
        value = jnp.dot(
            beta[at_row(which * half + c, chunk), :], wv[...], preferred_element_type=F32
        )
        if index + 1 < len(steps):
            projectors(*steps[index + 1][:2])
        if away:
            part[c : c + chunk, :] = value.astype(BF)
            if index == 0:
                @pl.when(side == 0)
                def _():
                    pl.semaphore_wait(here.at[mate], 1)
            swap(c).start()
        else:
            kept[c : c + chunk, :] = value
    for c in range(0, half, chunk):
        swap(c).wait_recv()
        pair_sum[c : c + chunk, :] = (
            kept[c : c + chunk, :] + pair_in[c : c + chunk, :].astype(F32)
        ).astype(BF)
        for z in range(single + double):
            if c <= first_slot(z) * rows < c + chunk:
                @pl.when(z < chip)
                def _():
                    scatter(z).start()

    beta_t[:, 0:every] = beta[:, 0:npw].T
    beta_t[:, every : 2 * every] = beta[:, npw : 2 * npw].T
    weights = occ[...] * (1.0 / (bands * nb))
    weights = jnp.concatenate([weights, weights], axis=1)
    group = min(atoms, 32)
    span = group * 8
    fan = (iota((8, span), 1) % 8 == iota((8, span), 0)).astype(F32)
    diagonal = iota((span, span), 0) // 8 == iota((span, span), 1) // 8
    fold = (iota((span, 8), 0) % 8 == iota((span, 8), 1)).astype(F32)
    slot = [iota((8, 128), 0) == 2 * t + iota((8, 128), 1) // 64 for t in range(4)]
    for kind in range(kinds):
        spread[kind] = jnp.dot(base[kind], fan, precision=HIGH, preferred_element_type=F32)
        for t in range(4):
            turned[kind, :, t * 128 : t * 128 + 128] = jnp.concatenate(
                [coupling[kind, i * 8 : i * 8 + 8, :] for i in (2 * t, 2 * t + 1)], axis=1
            )

    for k in range(0, atoms, 2):
        kind = [species[atom_at(k + e)] for e in range(2)]
        respond_t[k * 8 : k * 8 + 16, :] = jnp.concatenate(
            [turned[s] for s in kind], axis=0
        ).astype(BF)
        bare[k * 8 : k * 8 + 16, :] = jnp.concatenate([spread[s] for s in kind], axis=0)
    for q in range(0, every, span):
        respond[:, q : q + span] = respond_t[q : q + span, :].T

    for to in range(1, n):
        @pl.when(jnp.logical_and(to > me, to != mate))
        def _():
            pl.semaphore_wait(here.at[to], 1)

        if to // 2 < single + double:
            @pl.when(jnp.logical_and(to // 2 > chip, to % 2 == side))
            def _():
                scatter(to // 2).start()

    @pl.when(me == hub)
    def _():
        @pl.when(mb < nb - 1)
        def _():
            pl.semaphore_wait(here_b, nb - 1 - mb)

        for to in group_bands:
            pl.semaphore_signal(ready, inc=1, device_id={"band": to}, device_id_type=MESH)
        pl.semaphore_wait(ready, nb - 1)
        for to in others:
            pl.semaphore_signal(go, inc=1, device_id={"pw": to}, device_id_type=MESH)

    def skip(i, at, size):
        return i + (i + size - at) // size

    def occupancy_copy(to, band, at, first, count):
        return pltpu.make_async_remote_copy(
            src_ref=o_in.at[pl.ds(mb * n + first, count)],
            dst_ref=o_in.at[pl.ds(mb * n + first, count)],
            send_sem=oc_s.at[at],
            recv_sem=oc_r,
            device_id={"pw": to, "band": band},
            device_id_type=MESH,
        )

    def away(i, j):
        return skip(i, me, n), j

    def near(j):
        return me, skip(j, mb, nb)

    def each_peer(step):
        if peers <= 64:
            for i in range(n - 1):
                for j in range(nb):
                    step(*away(i, j), i * nb + j)
        else:
            lax.fori_loop(
                0, (n - 1) * nb, lambda q, c: (step(*away(q // nb, lax.rem(q, nb)), q), c)[1], 0
            )
        for j in range(nb - 1):
            step(*near(j), (n - 1) * nb + j)

    def projection_copy(i, first, count):
        at = at_row(first * rows, count * rows)
        return pltpu.make_async_remote_copy(
            src_ref=p_all.at[at],
            dst_ref=p_all.at[at],
            send_sem=ag_s.at[i],
            recv_sem=ag_r,
            device_id={"pw": skip(i, me, n)},
            device_id_type=MESH,
        )

    def own_first(count):
        return side * chips + (chip if count == 1 else 2 * chip - single)

    def each_role(act):
        for count, role in (
            (1, chip < single),
            (2, jnp.logical_and(chip >= single, chip < single + double)),
            (0, chip >= single + double),
        ):
            @pl.when(role)
            def _():
                act(count)

    def wait_go():
        @pl.when(me != hub)
        def _():
            pl.semaphore_wait(go, 1)

    def share(count):
        if count == 0:
            wait_go()
            return
        first, size = own_first(count), count * rows
        total = pair_sum[at_row((first - side * chips) * rows, size), :].astype(F32)
        for d in range(1, chips):
            z = lax.rem(chip + d, chips)
            pltpu.make_async_remote_copy(
                src_ref=rs_in.at[z, pl.ds(0, size)],
                dst_ref=rs_in.at[z, pl.ds(0, size)],
                send_sem=rs_s.at[z],
                recv_sem=rs_r.at[z],
                device_id={"pw": 2 * z + side},
                device_id_type=MESH,
            ).wait_recv()
            total = total + rs_in[z, 0:size, :].astype(F32)
        p_all[at_row(first * rows, size), :] = total.astype(BF)
        pairs = []
        for k in range(0, size, 8):
            left = total[k : k + 8, :] * weights
            pair = jnp.concatenate(
                [jnp.broadcast_to(total[k + i : k + i + 1, :], (8, 2 * bands)) * left for i in range(8)],
                axis=0,
            ).astype(BF)
            pairs += [pair, pair]
        flat = lax.dot_general(
            jnp.ones((16, 2 * bands), BF),
            jnp.concatenate(pairs, axis=0),
            (((1,), (1,)), ((), ())),
            preferred_element_type=F32,
        )
        for k in range(count * own):
            o_in[mb * n + first + k // own, k % own : k % own + 1, :] = flat[0:1, k * 128 : k * 128 + 128]
        wait_go()
        each_peer(lambda to, band, at: occupancy_copy(to, band, at, first, count).start())
        for i in range(n - 1):
            projection_copy(i, first, count).start()

    each_role(share)
    for c in range(0, half, chunk):
        swap(c).wait_send()
    for z in range(single + double):
        @pl.when(z != chip)
        def _():
            scatter(z).wait_send()

    def drain(count):
        if count:
            first = own_first(count)
            each_peer(lambda to, band, at: occupancy_copy(to, band, at, first, count).wait_send())
            for i in range(n - 1):
                projection_copy(i, first, count).wait_send()

    each_role(drain)
    def wait_occupancies(count):
        pltpu.make_async_copy(
            o_in.at[pl.ds(0, nb * n - count)], o_in.at[pl.ds(0, nb * n - count)], oc_r
        ).wait()

    each_role(wait_occupancies)
    for d in range(n):
        summed = o_in[d]
        for b in range(1, nb):
            summed = summed + o_in[b * n + d]
        o_sum[d * own : d * own + own, :] = summed
    matrix = []
    for q in range(0, atoms, group):
        lines = []
        for k in range(q, q + group):
            line = jnp.broadcast_to(o_sum[k : k + 1, :], (8, 128))
            lines.append(
                jnp.concatenate([jnp.where(slot[t], line, 0.0) for t in range(4)], axis=1)
            )
        lines = jnp.concatenate(lines, axis=0).astype(BF)
        answer = jnp.dot(
            lines, respond[:, q * 8 : q * 8 + span], preferred_element_type=F32
        )
        answer = jnp.where(diagonal, answer + bare[q * 8 : q * 8 + span, :], 0.0)
        folded[q * 8 : q * 8 + span, :] = answer
        matrix.append(answer.astype(BF))
    def wait_projections(count):
        got = p_all.at[pl.ds(0, every - count * rows)]
        pltpu.make_async_copy(got, got, ag_r).wait()

    each_role(wait_projections)
    for q in range(0, every, span):
        w = jnp.dot(matrix[q // span], p_all[q : q + span, :], preferred_element_type=F32)
        w = w.astype(BF)
        ww[q : q + span, :] = w
        ww[every + q : every + q + span, 0:bands] = -w[:, bands : 2 * bands]
        ww[every + q : every + q + span, bands : 2 * bands] = w[:, 0:bands]
    result = jnp.dot(beta_t[...], ww[...], preferred_element_type=F32).astype(BF)
    applied[0] = result[:, 0:bands]
    applied[1] = result[:, bands : 2 * bands]
    mine = jnp.dot(folded[at_row((side * chips + chip) * rows, rows), :], fold, precision=HIGH, preferred_element_type=F32)
    for k in range(own):
        onsite[k] = mine[k * 8 : k * 8 + 8, :]


def finish(applied_in, onsite_in, applied, onsite, sem):
    copies = [
        pltpu.make_async_copy(applied_in, applied, sem.at[0]),
        pltpu.make_async_copy(onsite_in, onsite, sem.at[1]),
    ]
    for copy in copies:
        copy.start()
    for copy in copies:
        copy.wait()


def solution(mesh):
    n, nb = mesh.shape["pw"], mesh.shape["band"]

    def local(wave, miller, reciprocal, fractional, species, order, widths, base, coupling, occ):
        _, npw, bands = wave.shape
        atoms = order.shape[0]
        own = atoms // n
        rows, every = own * 8, atoms * 8
        span = min(atoms, 32) * 8
        half = every // 2
        kinds = widths.shape[0]
        vmem = pl.BlockSpec(memory_space=pltpu.VMEM)
        hbm = pl.BlockSpec(memory_space=pltpu.HBM)
        dma = pltpu.SemaphoreType.DMA
        results = (
            jax.ShapeDtypeStruct(wave.shape, BF),
            jax.ShapeDtypeStruct((own, 8, 8), F32),
        )
        first = pl.pallas_call(
            functools.partial(kernel, n, nb),
            out_shape=results,
            in_specs=[hbm] * 10,
            out_specs=(vmem, vmem),
            scratch_shapes=[
                pltpu.VMEM(miller.shape, jnp.int32),
                pltpu.SMEM(reciprocal.shape, F32),
                pltpu.SMEM(fractional.shape, F32),
                pltpu.SMEM(species.shape, jnp.int32),
                pltpu.SMEM(order.shape, jnp.int32),
                pltpu.SMEM(widths.shape, F32),
                pltpu.VMEM(base.shape, F32),
                pltpu.VMEM(coupling.shape, F32),
                pltpu.VMEM((1, bands), F32),
                pltpu.VMEM((2 * npw, 2 * bands), BF),
                pltpu.VMEM((atoms, npw), F32),
                pltpu.VMEM((atoms, npw), F32),
                pltpu.VMEM((atoms, npw), F32),
                pltpu.VMEM((kinds, 8, npw), F32),
                pltpu.VMEM((every, 2 * npw), BF),
                pltpu.VMEM((npw, 2 * every), BF),
                pltpu.VMEM((half, 2 * bands), BF),
                pltpu.VMEM((half, 2 * bands), F32),
                pltpu.VMEM((half, 2 * bands), BF),
                pltpu.VMEM((half, 2 * bands), BF),
                pltpu.VMEM((n // 2, 2 * rows, 2 * bands), BF),
                pltpu.VMEM((every, 2 * bands), BF),
                pltpu.VMEM((nb * n, own, 128), F32),
                pltpu.VMEM((atoms, 128), F32),
                pltpu.VMEM((kinds, 8, span), F32),
                pltpu.VMEM((kinds, 8, 512), F32),
                pltpu.VMEM((every, 512), BF),
                pltpu.VMEM((512, every), BF),
                pltpu.VMEM((every, span), F32),
                pltpu.VMEM((every, span), F32),
                pltpu.VMEM((2 * every, 2 * bands), BF),
                dma((12,)),
                dma((half // (2 * rows),)),
                dma((half // (2 * rows),)),
                dma((n // 2,)),
                dma((n // 2,)),
                dma((n,)),
                dma,
                dma((n * nb,)),
                dma,
                pltpu.SemaphoreType.REGULAR,
                pltpu.SemaphoreType.REGULAR((n,)),
                pltpu.SemaphoreType.REGULAR,
                pltpu.SemaphoreType.REGULAR,
            ],
            compiler_params=pltpu.CompilerParams(
                collective_id=0, has_side_effects=True, vmem_limit_bytes=40 * 2**20
            ),
        )(
            *[
                pltpu.with_memory_space_constraint(value, pltpu.HBM)
                for value in (
                    wave,
                    miller,
                    reciprocal,
                    fractional,
                    species,
                    order,
                    widths,
                    base,
                    coupling,
                    occ.reshape(1, bands),
                )
            ]
        )
        anywhere = pl.BlockSpec(memory_space=pl.ANY)
        return pl.pallas_call(
            finish,
            out_shape=results,
            in_specs=[anywhere] * 2,
            out_specs=(hbm, hbm),
            scratch_shapes=[dma((2,))],
            compiler_params=pltpu.CompilerParams(vmem_limit_bytes=2**20),
        )(*first)

    placed = (P(None, "pw", "band"), P(None, "pw"), P(), P(), P(), P(), P(), P(), P(), P("band"))
    return jax.shard_map(
        local,
        mesh=mesh,
        in_specs=placed,
        out_specs=(P(None, "pw", "band"), P("pw", None, None)),
        check_vma=False,
    )
```
